32 devices in a mesh: lat: 8 (over y, x, core), lon: 4 (over z).
Axes of the slice: x: 2, y: 2, z: 4, core: 2. Of those that a mesh axis runs over, the one named last changes fastest.
Arguments:
- fields: float32 [4, 6, 256, 1280], P(None, None, 'lat', 'lon'), may hold values from -6 to 6
- dep_row: int32 [6, 256, 1280], P(None, 'lat', 'lon'), may hold values from -4 to 255, as said below
- dep_col: int32 [6, 256, 1280], P(None, 'lat', 'lon'), may hold values from 0 to 1279, as said below
- weights: float32 [8, 6, 256, 1280], P(None, None, 'lat', 'lon'), may hold values from -0.25 to 0.75
Outputs:
- departed: float32 [4, 6, 256, 1280], P(None, None, 'lat', 'lon')
The draws below stay inside these ranges and needn't reach their ends.
Inputs may be any that keep to these rules, and one draw needn't show every extreme that they name: dep_row[l, i, j] lies within i - 4 to i. dep_col[l, i, j] equals (j + k) modulo 1280 for some k from -4 to 0.
All inputs are finite; a program needn't handle non-finite values.
Results may differ from the reference program's by a relative error of at most 0.0003.
Values sent between devices are 32-bit elements; how exact they have to be, the bound alone decides.
A program may use at most 64 MiB of HBM per device.

```python
import jax
import jax.numpy as jnp
from jax import lax

LEV = 6
FIELDS = 4
HALO = 4
NR = 256
NC = 1280


def departures(key):
    base_key = jax.random.fold_in(key, 7713)
    key_rows, key_cols = jax.random.split(base_key)
    shape = (LEV, NR, NC)
    shift_rows = jax.random.randint(key_rows, shape, -3, 2, dtype=jnp.int32)
    shift_cols = jax.random.randint(key_cols, shape, -3, 2, dtype=jnp.int32)
    row_index = lax_iota(shape, 1)
    col_index = lax_iota(shape, 2)
    rows = row_index + shift_rows - 1
    cols = jnp.mod(col_index + shift_cols - 1, NC)
    return (rows.astype(jnp.int32), cols.astype(jnp.int32))


def lax_iota(shape, dim):
    return jax.lax.broadcasted_iota(jnp.int32, shape, dim)


def draw_dep_row(key, part):
    return departures(key)[0]


def draw_dep_col(key, part):
    return departures(key)[1]


def block_levels(stream_key, dims, cuts, least, top_value):
    gain, own = 1.0, jax.random.fold_in(stream_key, 6)
    for dim, blocks in cuts:
        steps = jnp.exp(jax.random.uniform(jax.random.fold_in(own, dim), (blocks,), jnp.float32, least / len(cuts), top_value / len(cuts)))
        gain = gain * jnp.repeat(steps, dims[dim] // blocks).reshape([-1 if axis == dim else 1 for axis in range(len(dims))])
    return gain


def bell_draw(own_key, extent, deviation, most, pieces=(), held_as=jnp.bfloat16):
    drawn = deviation * jax.random.normal(own_key, extent, jnp.float32)
    if pieces:
        drawn = drawn * block_levels(own_key, extent, pieces, -0.22, 0.18)
    return jnp.clip(drawn, -most, most).astype(held_as)


def setup_inputs(seed: int = 0) -> dict:
    key_of = jax.random.split(jax.random.key(seed), 5)
    return {
        "fields": bell_draw(key_of[0], (FIELDS, LEV, NR, NC), 1.0, 6.0, ((2, 8), (3, 4)), jnp.float32),
        "dep_row": draw_dep_row(jax.random.fold_in(key_of[4], 71), 0),
        "dep_col": draw_dep_col(jax.random.fold_in(key_of[4], 71), 0),
        "weights": jnp.clip(-0.25 + 1.0 * jax.random.uniform(key_of[3], (8, LEV, NR, NC), jnp.float32) ** block_levels(key_of[3], (8, LEV, NR, NC), ((2, 8), (3, 4)), -0.2, 0.2), -0.25, 0.75),
    }


def interpolate_level(item):
    field, rows, cols, weight = item
    half = NC // 2
    north = jnp.roll(field[:, :HALO][:, ::-1], half, axis=2)
    south = jnp.roll(field[:, NR - HALO:][:, ::-1], half, axis=2)
    tall = jnp.concatenate([north, field, south], axis=1)
    padded = jnp.concatenate([tall[:, :, NC - HALO:], tall, tall[:, :, :HALO]], axis=2)
    width = NC + 2 * HALO
    flat = padded.reshape(FIELDS, -1)
    base = ((rows + HALO) * width + (cols + HALO)).astype(jnp.int32).reshape(-1)
    total = jnp.zeros((FIELDS, NR * NC), jnp.float32)
    for first in range(4):
        line = jnp.zeros((FIELDS, NR * NC), jnp.float32)
        for second in range(4):
            values = jnp.take(flat, base + first * width + second, axis=1)
            line = line + weight[4 + second].reshape(1, -1) * values
        total = total + weight[first].reshape(1, -1) * line
    return total.reshape(FIELDS, NR, NC)


def reference(fields, dep_row, dep_col, weights):
    result = lax.map(interpolate_level, (jnp.transpose(fields, (1, 0, 2, 3)), dep_row, dep_col, jnp.transpose(weights, (1, 0, 2, 3))))
    return jnp.transpose(result, (1, 0, 2, 3))
```

```python
import functools

import jax
import jax.numpy as jnp
from jax import lax
from jax.experimental import pallas as pl
from jax.experimental.pallas import tpu as pltpu
from jax.sharding import PartitionSpec as P

HALO = 4
LANES = 128
SUB = 8
CHUNK = LANES - 2 * HALO
NSHIFT = 2 * HALO


def beside(x, axis, dim, width, wrap):
    devices, length = (lax.axis_size(axis), x.shape[dim])
    up = [(i, (i + 1) % devices) for i in range(devices if wrap else devices - 1)]
    down = [(j, i) for i, j in up]
    last = lax.slice_in_dim(x, length - width, length, axis=dim)
    leading = lax.slice_in_dim(x, 0, width, axis=dim)
    return lax.ppermute(last, axis, up), lax.ppermute(leading, axis, down)


def swapped(x, axis, stride):
    return lax.ppermute(x, axis, [(i, i ^ 1 << stride) for i in range(lax.axis_size(axis))])


def lane_index():
    return lax.broadcasted_iota(jnp.int32, (SUB, LANES), 1)


def chunked(tiles, side=None):
    lane = lane_index()
    out = [tiles[0] if side is None else jnp.where(lane < LANES - HALO, tiles[0], side)]
    for t in range(1, len(tiles)):
        back = (LANES - CHUNK) * t
        mixed = jnp.where(lane < LANES - HALO - back, tiles[t], tiles[t - 1])
        out.append(pltpu.roll(mixed, back, 1))
    return out


def unchunked(chunks):
    lane = lane_index()
    count = len(chunks)
    ahead = [c if t == 0 else pltpu.roll(c, LANES - (LANES - CHUNK) * t, 1) for t, c in enumerate(chunks)]
    return [
        ahead[t] if t == count - 1 else jnp.where(lane < CHUNK - (LANES - CHUNK) * t, ahead[t], ahead[t + 1])
        for t in range(count)
    ]


def spread(offset, w):
    one, two, four = (offset & 1) != 0, (offset & 2) != 0, offset == 4
    zero = jnp.zeros_like(w[0])
    u = [jnp.where(one, a, b) for a, b in zip([zero] + w, w + [zero])]
    v = [jnp.where(two, a, b) for a, b in zip([zero, zero] + u, u + [zero, zero])]
    return [jnp.where(four, a, b) for a, b in zip([zero] * 4 + w, v + [zero])]


def stencil(cols, total_cols, fields_ref, row_ref, col_ref, weight_ref, side_ref, caps_ref, out_ref, xs, sel, res):
    nfield, rows = fields_ref.shape[0], fields_ref.shape[2]
    tiles = pl.cdiv(cols, LANES)
    groups = rows // SUB
    row0 = lax.axis_index("lat") * rows
    col0 = lax.axis_index("lon") * cols
    lane = lane_index()
    sub = lax.broadcasted_iota(jnp.int32, (SUB, LANES), 0)
    lanes_of = [pl.ds(LANES * t, LANES) for t in range(tiles)]

    for i in range(groups):
        span = pl.ds(SUB * i, SUB)
        offsets = []
        for t in range(tiles):
            o_row = row_ref[0, span, lanes_of[t]] - (row0 + SUB * i + sub) + HALO
            back = col_ref[0, span, lanes_of[t]] - (col0 + LANES * t + lane)
            o_col = jnp.where(back > 0, back - total_cols, back) + HALO
            offsets.append(o_row * 16 + o_col)
        offsets = chunked(offsets)
        w = [chunked([weight_ref[q, 0, span, at] for at in lanes_of]) for q in range(8)]
        for t in range(tiles):
            for base, offset in ((0, offsets[t] >> 4), (4, offsets[t] & 15)):
                slots = spread(offset, [w[base + a][t] for a in range(4)])
                for s in range(NSHIFT):
                    sel[2 * base + s, t, span, :] = slots[s]

    for f in range(nfield):
        for i in range(groups):
            span = pl.ds(SUB * i, SUB)
            side = side_ref[f, 0, span, :]
            got = [fields_ref[f, 0, span, at] for at in lanes_of]
            got[-1] = jnp.where(lane < cols - LANES * (tiles - 1), got[-1], side)
            for t, chunk in enumerate(chunked(got, side)):
                xs[f, t, pl.ds(SUB * (i + 1), SUB), :] = chunk
        got = [caps_ref[f, 0, :, at] for at in lanes_of]
        for t, chunk in enumerate(chunked(got, got[-1])):
            xs[f, t, pl.ds(0, SUB), :] = chunk
            xs[f, t, pl.ds(SUB * (groups + 1), SUB), :] = chunk

    stride = rows // SUB
    many = 2 if stride % 2 == 0 else 1
    pair = 2 if nfield % 2 == 0 else 1
    for t in range(tiles):
        for m0 in range(0, stride, many):
            rowsel = [
                [sel[r, t, pl.ds(m0 + m, SUB, stride=stride), :] for r in range(NSHIFT)] for m in range(many)
            ]
            for f0 in range(0, nfield, pair):
                total = [[None] * pair for _ in range(many)]
                for s in range(NSHIFT):
                    colsel = [sel[NSHIFT + s, t, pl.ds(m0 + m, SUB, stride=stride), :] for m in range(many)]
                    for f in range(pair):
                        x = []
                        for r in range(many + NSHIFT - 1):
                            value = xs[f0 + f, t, pl.ds(HALO + m0 + r, SUB, stride=stride), :]
                            x.append(value if s == HALO else pltpu.roll(value, (HALO - s) % LANES, 1))
                        for m in range(many):
                            line = rowsel[m][0] * x[m]
                            for r in range(1, NSHIFT):
                                line = line + rowsel[m][r] * x[m + r]
                            term = colsel[m] * line
                            total[m][f] = term if s == 0 else total[m][f] + term
                for m in range(many):
                    for f in range(pair):
                        res[f0 + f, t, pl.ds(m0 + m, SUB, stride=stride), :] = total[m][f]
    for f in range(nfield):
        for i in range(groups):
            span = pl.ds(SUB * i, SUB)
            for t, tile in enumerate(unchunked([res[f, t, span, :] for t in range(tiles)])):
                out_ref[f, 0, span, lanes_of[t]] = tile


def halos(fields):
    nfield, nlev, rows, cols = fields.shape
    band, lat_count, lon_count = lax.axis_index("lat"), lax.axis_size("lat"), lax.axis_size("lon")
    west, east = beside(fields, "lon", 3, HALO, True)
    wide = jnp.concatenate([west, fields, east], axis=3)
    from_north, from_south = beside(wide, "lat", 2, HALO, False)
    outgoing = jnp.where(band == 0, wide[:, :, :HALO], wide[:, :, rows - HALO :])
    flipped = swapped(outgoing, "lon", lon_count.bit_length() - 2)[:, :, ::-1]
    north = jnp.where(band == 0, flipped, from_north)
    south = jnp.where(band == lat_count - 1, flipped, from_south)
    last = LANES * ((cols - 1) // LANES)

    def gap(h, n):
        return jnp.zeros((nfield, nlev, h, n), jnp.float32)

    tail = last + LANES - cols - 2 * HALO
    side = jnp.concatenate([gap(rows, cols - last), east, gap(rows, tail), west], axis=3)
    caps = jnp.concatenate([south, north], axis=2)
    caps = jnp.concatenate([caps[..., HALO:], gap(2 * HALO, tail), caps[..., :HALO]], axis=3)
    return side, caps


def body(fields, dep_row, dep_col, weights):
    nfield, nlev, rows, cols = fields.shape
    side, caps = halos(fields)
    tiles = pl.cdiv(cols, LANES)
    wide = tiles * LANES
    assert rows % SUB == 0 and CHUNK * tiles >= cols and cols + 2 * HALO <= wide

    def block(lead, h, w):
        return pl.BlockSpec((lead, 1, h, w), lambda l: (0, l, 0, 0))

    point = pl.BlockSpec((1, rows, wide), lambda l: (l, 0, 0))
    return pl.pallas_call(
        functools.partial(stencil, cols, cols * lax.axis_size("lon")),
        grid=(nlev,),
        out_shape=jax.ShapeDtypeStruct(fields.shape, jnp.float32),
        in_specs=[
            block(nfield, rows, wide),
            point,
            point,
            block(8, rows, wide),
            block(nfield, rows, LANES),
            block(nfield, 2 * HALO, wide),
        ],
        out_specs=block(nfield, rows, wide),
        scratch_shapes=[
            pltpu.VMEM((nfield, tiles, rows + 2 * SUB, LANES), jnp.float32),
            pltpu.VMEM((2 * NSHIFT, tiles, rows, LANES), jnp.float32),
            pltpu.VMEM((nfield, tiles, rows, LANES), jnp.float32),
        ],
    )(fields, dep_row, dep_col, weights, side, caps)


def solution(mesh):
    return jax.shard_map(
        body,
        mesh=mesh,
        in_specs=(
            P(None, None, "lat", "lon"),
            P(None, "lat", "lon"),
            P(None, "lat", "lon"),
            P(None, None, "lat", "lon"),
        ),
        out_specs=P(None, None, "lat", "lon"),
        check_vma=False,
    )
```

```python
import functools

import jax
import jax.numpy as jnp
from jax import lax
from jax.experimental import pallas as pl
from jax.experimental.pallas import tpu as pltpu
from jax.sharding import PartitionSpec as P

HALO = 4
LANES = 128
SUB = 8
CHUNK = LANES - 2 * HALO
NSHIFT = 2 * HALO


def lane_index():
    return lax.broadcasted_iota(jnp.int32, (SUB, LANES), 1)


def sublane_index():
    return lax.broadcasted_iota(jnp.int32, (SUB, LANES), 0)


def chunked(tiles, side=None):
    lane = lane_index()
    out = [tiles[0] if side is None else jnp.where(lane < LANES - HALO, tiles[0], side)]
    for t in range(1, len(tiles)):
        back = (LANES - CHUNK) * t
        mixed = jnp.where(lane < LANES - HALO - back, tiles[t], tiles[t - 1])
        out.append(pltpu.roll(mixed, back, 1))
    return out


def unchunked(chunks):
    lane = lane_index()
    count = len(chunks)
    ahead = [c if t == 0 else pltpu.roll(c, LANES - (LANES - CHUNK) * t, 1) for t, c in enumerate(chunks)]
    return [
        ahead[t] if t == count - 1 else jnp.where(lane < CHUNK - (LANES - CHUNK) * t, ahead[t], ahead[t + 1])
        for t in range(count)
    ]


def spread(offset, w):
    one, two, four = (offset & 1) != 0, (offset & 2) != 0, offset == 4
    zero = jnp.zeros_like(w[0])
    u = [jnp.where(one, a, b) for a, b in zip([zero] + w, w + [zero])]
    v = [jnp.where(two, a, b) for a, b in zip([zero, zero] + u, u + [zero, zero])]
    return [jnp.where(four, a, b) for a, b in zip([zero] * 4 + w, v + [zero])]


def stencil(cols, total_cols, fields_ref, row_ref, col_ref, weight_ref, west_ref, east_ref, rows_ref, corner_ref, out_ref, xs, sel, res):
    nfield, rows = fields_ref.shape[0], fields_ref.shape[2]
    tiles = pl.cdiv(cols, LANES)
    groups = rows // SUB
    row0 = lax.axis_index("lat") * rows
    col0 = lax.axis_index("lon") * cols
    level = pl.program_id(0)
    held = cols - LANES * (tiles - 1)
    lane, sub = lane_index(), sublane_index()
    top, bottom = lax.axis_index("lat") == 0, lax.axis_index("lat") == lax.axis_size("lat") - 1
    turned = ((sub < HALO) & bottom) | ((sub >= HALO) & top)
    lanes_of = [pl.ds(LANES * t, LANES) for t in range(tiles)]

    for i in range(groups):
        span = pl.ds(SUB * i, SUB)
        offsets = []
        for t in range(tiles):
            o_row = row_ref[0, span, lanes_of[t]] - (row0 + SUB * i + sub) + HALO
            back = col_ref[0, span, lanes_of[t]] - (col0 + LANES * t + lane)
            o_col = jnp.where(back > 0, back - total_cols, back) + HALO
            offsets.append(o_row * 16 + o_col)
        offsets = chunked(offsets)
        w = [chunked([weight_ref[q, 0, span, at] for at in lanes_of]) for q in range(8)]
        for t in range(tiles):
            for base, offset in ((0, offsets[t] >> 4), (4, offsets[t] & 15)):
                slots = spread(offset, [w[base + a][t] for a in range(4)])
                for s in range(NSHIFT):
                    sel[2 * base + s, t, span, :] = slots[s]

    corner = []
    for k in range(2):
        north, south = corner_ref[k, 0], corner_ref[k, 1]
        north = jnp.where(top, pltpu.roll(north, HALO, 0), north)
        south = jnp.where(bottom, pltpu.roll(south, HALO, 0), south)
        corner.append(jnp.where(sub < HALO, south, north))

    for f in range(nfield):
        place = HALO * (level * nfield + f)

        def flanks(west, east):
            west = pltpu.roll(west, LANES - HALO - place, 1)
            east = pltpu.roll(east, lax.rem(LANES + held - place, LANES), 1)
            return jnp.where(lane < LANES - HALO, east, west)

        for i in range(groups):
            span = pl.ds(SUB * i, SUB)
            side = flanks(west_ref[span, :], east_ref[span, :])
            got = [fields_ref[f, 0, span, at] for at in lanes_of]
            got[-1] = jnp.where(lane < held, got[-1], side)
            for t, chunk in enumerate(chunked(got, side)):
                xs[f, t, pl.ds(SUB * (i + 1), SUB), :] = chunk
        got = []
        for at in lanes_of:
            north, south = (rows_ref[n, 0, f // 2, :, at] for n in range(2))
            if f % 2 == 0:
                north = pltpu.roll(north, HALO, 0)
            else:
                south = pltpu.roll(south, HALO, 0)
            got.append(jnp.where(sub < HALO, south, north))
        got[-1] = jnp.where(lane < held, got[-1], flanks(*corner))
        for t in range(tiles):
            back = got[t]
            for step in (1, 2):
                back = jnp.where((sub & step) != 0, pltpu.roll(back, step, 0), pltpu.roll(back, SUB - step, 0))
            got[t] = jnp.where(turned, back, got[t])
        for t, chunk in enumerate(chunked(got, got[-1])):
            xs[f, t, pl.ds(0, SUB), :] = chunk
            xs[f, t, pl.ds(SUB * (groups + 1), SUB), :] = chunk

    stride = rows // SUB
    many = 2 if stride % 2 == 0 else 1
    pair = 2 if nfield % 2 == 0 else 1
    for t in range(tiles):
        for m0 in range(0, stride, many):
            rowsel = [
                [sel[r, t, pl.ds(m0 + m, SUB, stride=stride), :] for r in range(NSHIFT)] for m in range(many)
            ]
            for f0 in range(0, nfield, pair):
                total = [[None] * pair for _ in range(many)]
                for s in range(NSHIFT):
                    colsel = [sel[NSHIFT + s, t, pl.ds(m0 + m, SUB, stride=stride), :] for m in range(many)]
                    for f in range(pair):
                        x = []
                        for r in range(many + NSHIFT - 1):
                            value = xs[f0 + f, t, pl.ds(HALO + m0 + r, SUB, stride=stride), :]
                            x.append(value if s == HALO else pltpu.roll(value, (HALO - s) % LANES, 1))
                        for m in range(many):
                            line = rowsel[m][0] * x[m]
                            for r in range(1, NSHIFT):
                                line = line + rowsel[m][r] * x[m + r]
                            term = colsel[m] * line
                            total[m][f] = term if s == 0 else total[m][f] + term
                for m in range(many):
                    for f in range(pair):
                        res[f0 + f, t, pl.ds(m0 + m, SUB, stride=stride), :] = total[m][f]
    for f in range(nfield):
        for i in range(groups):
            span = pl.ds(SUB * i, SUB)
            for t, tile in enumerate(unchunked([res[f, t, span, :] for t in range(tiles)])):
                out_ref[f, 0, span, lanes_of[t]] = tile


def exchange(cols, fields_ref, west_ref, east_ref, rows_ref, corner_ref, edge, ends, side, far, near, send, recv):
    nfield, nlev, rows = fields_ref.shape[:3]
    tiles = pl.cdiv(cols, LANES)
    last = LANES * (tiles - 1)
    lat_count, lon_count = lax.axis_size("lat"), lax.axis_size("lon")
    band, sector = lax.axis_index("lat"), lax.axis_index("lon")
    lane, sub = lane_index(), sublane_index()
    top, bottom = band == 0, band == lat_count - 1
    across = lax.rem(sector + lon_count // 2, lon_count)
    up = (jnp.maximum(band - 1, 0), jnp.where(top, across, sector))
    down = (jnp.minimum(band + 1, lat_count - 1), jnp.where(bottom, across, sector))
    slot_up, slot_down = jnp.where(top, 0, 1), jnp.where(bottom, 1, 0)

    def ahead(where, step):
        return (where[0], lax.rem(where[1] + step + lon_count, lon_count))

    here = (band, sector)
    targets = [ahead(here, 1), ahead(here, -1)]
    for where in (up, down):
        targets += [where, ahead(where, 1), ahead(where, -1)]
    barrier = pltpu.get_barrier_semaphore()
    for target in targets:
        pl.semaphore_signal(barrier, inc=1, device_id=target, device_id_type=pl.DeviceIdType.MESH)

    for i in range(rows // SUB):
        span = pl.ds(SUB * i, SUB)
        packed = [jnp.zeros((SUB, LANES), jnp.float32)] * 2
        for l in range(nlev):
            for f in range(nfield):
                g = HALO * (l * nfield + f)
                mine = (lane >= g) & (lane < g + HALO)
                ending = fields_ref[f, l, span, pl.ds(last, LANES)]
                start = fields_ref[f, l, span, pl.ds(0, LANES)]
                shift = (g - (cols - last - HALO)) % LANES
                packed[0] = jnp.where(mine, pltpu.roll(ending, shift, 1) if shift else ending, packed[0])
                packed[1] = jnp.where(mine, pltpu.roll(start, g, 1) if g else start, packed[1])
        for k in range(2):
            edge[k, span, :] = packed[k]
    for l in range(nlev):
        for j in range(nfield // 2):
            for t in range(tiles):
                at = pl.ds(LANES * t, LANES)
                first = [fields_ref[2 * j + h, l, pl.ds(0, SUB), at] for h in range(2)]
                final = [fields_ref[2 * j + h, l, pl.ds(rows - SUB, SUB), at] for h in range(2)]
                ends[0, l, j, :, at] = jnp.where(sub < HALO, first[0], pltpu.roll(first[1], HALO, 0))
                ends[1, l, j, :, at] = jnp.where(sub < HALO, pltpu.roll(final[0], HALO, 0), final[1])
    pl.semaphore_wait(barrier, len(targets))

    copies = []

    def start_copy(source, dest, recv_sem, target):
        copy = pltpu.make_async_remote_copy(
            src_ref=source,
            dst_ref=dest,
            send_sem=send.at[len(copies)],
            recv_sem=recv_sem,
            device_id=target,
            device_id_type=pl.DeviceIdType.MESH,
        )
        copy.start()
        copies.append(copy)

    for k, (where, slot) in enumerate(((up, slot_up), (down, slot_down))):
        start_copy(ends.at[k], far.at[slot], recv.at[2 + slot], where)
    for k, step in enumerate((1, -1)):
        start_copy(edge.at[k], side.at[k], recv.at[k], ahead(here, step))
    for n, (where, slot) in enumerate(((up, slot_up), (down, slot_down))):
        span = pl.ds((rows - SUB) * n, SUB)
        for k, step in enumerate((1, -1)):
            start_copy(edge.at[k, span], near.at[k, slot], recv.at[4 + 2 * k + slot], ahead(where, step))
    for copy in copies:
        copy.wait_send()

    def arrived(dest, sem):
        pltpu.make_async_copy(dest, dest, recv.at[sem]).wait()

    for k in range(2):
        arrived(side.at[k], k)
        arrived(far.at[k], 2 + k)
        for n in range(2):
            arrived(near.at[k, n], 4 + 2 * k + n)
    west_ref[...] = side[0]
    east_ref[...] = side[1]
    corner_ref[...] = near[...]
    rows_ref[...] = far[...]


def halos(fields):
    nfield, nlev, rows, cols = fields.shape
    wide = pl.cdiv(cols, LANES) * LANES
    ends = (2, nlev, nfield // 2, SUB, wide)
    shapes = [(rows, LANES), (rows, LANES), ends, (2, 2, SUB, LANES)]

    def whole(shape):
        return pl.BlockSpec(shape, lambda n: (0,) * len(shape))

    return pl.pallas_call(
        functools.partial(exchange, cols),
        grid=(1,),
        out_shape=[jax.ShapeDtypeStruct(s, jnp.float32) for s in shapes],
        in_specs=[whole((nfield, nlev, rows, wide))],
        out_specs=[whole(s) for s in shapes],
        scratch_shapes=[
            pltpu.VMEM((2, rows, LANES), jnp.float32),
            pltpu.VMEM(ends, jnp.float32),
            pltpu.VMEM((2, rows, LANES), jnp.float32),
            pltpu.VMEM(ends, jnp.float32),
            pltpu.VMEM((2, 2, SUB, LANES), jnp.float32),
            pltpu.SemaphoreType.DMA((8,)),
            pltpu.SemaphoreType.DMA((8,)),
        ],
        compiler_params=pltpu.CompilerParams(collective_id=0, has_side_effects=True),
    )(fields)


def body(fields, dep_row, dep_col, weights):
    nfield, nlev, rows, cols = fields.shape
    west, east, ends, corners = halos(fields)
    tiles = pl.cdiv(cols, LANES)
    wide = tiles * LANES
    assert nfield % 2 == 0 and HALO * nfield * nlev <= LANES - HALO
    assert rows % SUB == 0 and CHUNK * tiles >= cols and cols + 2 * HALO <= wide

    def block(lead, h, w):
        return pl.BlockSpec((lead, 1, h, w), lambda l: (0, l, 0, 0))

    point = pl.BlockSpec((1, rows, wide), lambda l: (l, 0, 0))
    return pl.pallas_call(
        functools.partial(stencil, cols, cols * lax.axis_size("lon")),
        grid=(nlev,),
        out_shape=jax.ShapeDtypeStruct(fields.shape, jnp.float32),
        in_specs=[
            block(nfield, rows, wide),
            point,
            point,
            block(8, rows, wide),
            pl.BlockSpec((rows, LANES), lambda l: (0, 0)),
            pl.BlockSpec((rows, LANES), lambda l: (0, 0)),
            pl.BlockSpec((2, 1, nfield // 2, SUB, wide), lambda l: (0, l, 0, 0, 0)),
            pl.BlockSpec((2, 2, SUB, LANES), lambda l: (0, 0, 0, 0)),
        ],
        out_specs=block(nfield, rows, wide),
        scratch_shapes=[
            pltpu.VMEM((nfield, tiles, rows + 2 * SUB, LANES), jnp.float32),
            pltpu.VMEM((2 * NSHIFT, tiles, rows, LANES), jnp.float32),
            pltpu.VMEM((nfield, tiles, rows, LANES), jnp.float32),
        ],
    )(fields, dep_row, dep_col, weights, west, east, ends, corners)


def solution(mesh):
    return jax.shard_map(
        body,
        mesh=mesh,
        in_specs=(
            P(None, None, "lat", "lon"),
            P(None, "lat", "lon"),
            P(None, "lat", "lon"),
            P(None, None, "lat", "lon"),
        ),
        out_specs=P(None, None, "lat", "lon"),
        check_vma=False,
    )
```

```python
import functools

import jax
import jax.numpy as jnp
from jax import lax
from jax.experimental import pallas as pl
from jax.experimental.pallas import tpu as pltpu
from jax.sharding import PartitionSpec as P

HALO = 4
LANES = 128
SUB = 8
CHUNK = LANES - 2 * HALO
NSHIFT = 2 * HALO


def lane_index():
    return lax.broadcasted_iota(jnp.int32, (SUB, LANES), 1)


def sublane_index():
    return lax.broadcasted_iota(jnp.int32, (SUB, LANES), 0)


def chunked(tiles, side=None):
    lane = lane_index()
    out = [tiles[0] if side is None else jnp.where(lane < LANES - HALO, tiles[0], side)]
    for t in range(1, len(tiles)):
        back = (LANES - CHUNK) * t
        mixed = jnp.where(lane < LANES - HALO - back, tiles[t], tiles[t - 1])
        out.append(pltpu.roll(mixed, back, 1))
    return out


def unchunked(chunks):
    lane = lane_index()
    count = len(chunks)
    ahead = [c if t == 0 else pltpu.roll(c, LANES - (LANES - CHUNK) * t, 1) for t, c in enumerate(chunks)]
    return [
        ahead[t] if t == count - 1 else jnp.where(lane < CHUNK - (LANES - CHUNK) * t, ahead[t], ahead[t + 1])
        for t in range(count)
    ]


def spread(offset, w):
    one, two, four = (offset & 1) != 0, (offset & 2) != 0, offset == 4
    zero = jnp.zeros_like(w[0])
    u = [jnp.where(one, a, b) for a, b in zip([zero] + w, w + [zero])]
    v = [jnp.where(two, a, b) for a, b in zip([zero, zero] + u, u + [zero, zero])]
    return [jnp.where(four, a, b) for a, b in zip([zero] * 4 + w, v + [zero])]


def stencil(cols, total_cols, fields_ref, row_ref, col_ref, weight_ref, flank_ref, rows_ref, out_ref, xs, sel, res):
    nfield, rows = fields_ref.shape[0], fields_ref.shape[2]
    tiles = pl.cdiv(cols, LANES)
    groups = rows // SUB
    row0 = lax.axis_index("lat") * rows
    col0 = lax.axis_index("lon") * cols
    held = cols - LANES * (tiles - 1)
    lane, sub = lane_index(), sublane_index()
    top, bottom = lax.axis_index("lat") == 0, lax.axis_index("lat") == lax.axis_size("lat") - 1
    turned = ((sub < HALO) & bottom) | ((sub >= HALO) & top)
    lanes_of = [pl.ds(LANES * t, LANES) for t in range(tiles)]

    for i in range(groups):
        span = pl.ds(SUB * i, SUB)
        offsets = []
        for t in range(tiles):
            o_row = row_ref[0, span, lanes_of[t]] - (row0 + SUB * i + sub) + HALO
            back = col_ref[0, span, lanes_of[t]] - (col0 + LANES * t + lane)
            o_col = jnp.where(back > 0, back - total_cols, back) + HALO
            offsets.append(o_row * 16 + o_col)
        offsets = chunked(offsets)
        w = [chunked([weight_ref[q, 0, span, at] for at in lanes_of]) for q in range(8)]
        for t in range(tiles):
            for base, offset in ((0, offsets[t] >> 4), (4, offsets[t] & 15)):
                slots = spread(offset, [w[base + a][t] for a in range(4)])
                for s in range(NSHIFT):
                    sel[2 * base + s, t, span, :] = slots[s]

    def shifted(f, t, chunk, places):
        for s in range(NSHIFT):
            value = chunk if s == HALO else pltpu.roll(chunk, (HALO - s) % LANES, 1)
            for i in places:
                xs[f, s, t, pl.ds(SUB * i, SUB), :] = value

    for f in range(nfield):
        def flanks(i):
            return pltpu.roll(flank_ref[0, pl.ds(SUB * i, SUB), :], held - HALO * f, 1)

        for i in range(groups):
            span = pl.ds(SUB * i, SUB)
            side = flanks(i)
            got = [fields_ref[f, 0, span, at] for at in lanes_of]
            got[-1] = jnp.where(lane < held, got[-1], side)
            for t, chunk in enumerate(chunked(got, side)):
                shifted(f, t, chunk, (i + 1,))
        got = []
        for at in lanes_of:
            north, south = (rows_ref[n, 0, f // 2, :, at] for n in range(2))
            if f % 2 == 0:
                north = pltpu.roll(north, HALO, 0)
            else:
                south = pltpu.roll(south, HALO, 0)
            got.append(jnp.where(sub < HALO, south, north))
        got[-1] = jnp.where(lane < held, got[-1], flanks(groups))
        for t in range(tiles):
            back = got[t]
            for step in (1, 2):
                back = jnp.where((sub & step) != 0, pltpu.roll(back, step, 0), pltpu.roll(back, SUB - step, 0))
            got[t] = jnp.where(turned, back, got[t])
        for t, chunk in enumerate(chunked(got, got[-1])):
            shifted(f, t, chunk, (0, groups + 1))

    stride = rows // SUB
    many = 2 if stride % 2 == 0 else 1
    pair = 2 if nfield % 2 == 0 else 1
    def block(n, carry):
        f0, rest = pair * lax.rem(n, nfield // pair), n // (nfield // pair)
        m0, t = many * lax.rem(rest, stride // many), rest // (stride // many)
        rowsel = [[sel[r, t, pl.ds(m0 + m, SUB, stride=stride), :] for r in range(NSHIFT)] for m in range(many)]
        total = [[None] * pair for _ in range(many)]
        for s in range(NSHIFT):
            colsel = [sel[NSHIFT + s, t, pl.ds(m0 + m, SUB, stride=stride), :] for m in range(many)]
            for f in range(pair):
                x = [xs[f0 + f, s, t, pl.ds(HALO + m0 + r, SUB, stride=stride), :] for r in range(many + NSHIFT - 1)]
                for m in range(many):
                    line = rowsel[m][0] * x[m]
                    for r in range(1, NSHIFT):
                        line = line + rowsel[m][r] * x[m + r]
                    term = colsel[m] * line
                    total[m][f] = term if s == 0 else total[m][f] + term
        for m in range(many):
            for f in range(pair):
                res[f0 + f, t, pl.ds(m0 + m, SUB, stride=stride), :] = total[m][f]
        return carry

    lax.fori_loop(0, tiles * (stride // many) * (nfield // pair), block, 0)
    for f in range(nfield):
        for i in range(groups):
            span = pl.ds(SUB * i, SUB)
            for t, tile in enumerate(unchunked([res[f, t, span, :] for t in range(tiles)])):
                out_ref[f, 0, span, lanes_of[t]] = tile


def exchange(cols, fields_ref, flank_ref, rows_ref, edge, ends, side, far, near, send, recv):
    nfield, nlev, rows = fields_ref.shape[:3]
    tiles = pl.cdiv(cols, LANES)
    last = LANES * (tiles - 1)
    lat_count, lon_count = lax.axis_size("lat"), lax.axis_size("lon")
    band, sector = lax.axis_index("lat"), lax.axis_index("lon")
    lane, sub = lane_index(), sublane_index()
    top, bottom = band == 0, band == lat_count - 1
    across = lax.rem(sector + lon_count // 2, lon_count)
    up = (jnp.maximum(band - 1, 0), jnp.where(top, across, sector))
    down = (jnp.minimum(band + 1, lat_count - 1), jnp.where(bottom, across, sector))
    slot_up, slot_down = jnp.where(top, 0, 1), jnp.where(bottom, 1, 0)

    def ahead(where, step):
        return (where[0], lax.rem(where[1] + step + lon_count, lon_count))

    here = (band, sector)
    targets = [ahead(here, 1), ahead(here, -1)]
    for where in (up, down):
        targets += [where, ahead(where, 1), ahead(where, -1)]
    barrier = pltpu.get_barrier_semaphore()
    for target in targets:
        pl.semaphore_signal(barrier, inc=1, device_id=target, device_id_type=pl.DeviceIdType.MESH)

    for i in range(rows // SUB):
        span = pl.ds(SUB * i, SUB)
        packed = [jnp.zeros((SUB, LANES), jnp.float32)] * 2
        for l in range(nlev):
            for f in range(nfield):
                g = HALO * (l * nfield + f)
                mine = (lane >= g) & (lane < g + HALO)
                ending = fields_ref[f, l, span, pl.ds(last, LANES)]
                start = fields_ref[f, l, span, pl.ds(0, LANES)]
                shift = (g - (cols - last - HALO)) % LANES
                packed[0] = jnp.where(mine, pltpu.roll(ending, shift, 1) if shift else ending, packed[0])
                packed[1] = jnp.where(mine, pltpu.roll(start, g, 1) if g else start, packed[1])
        for k in range(2):
            edge[k, span, :] = packed[k]
    for l in range(nlev):
        for j in range(nfield // 2):
            for t in range(tiles):
                at = pl.ds(LANES * t, LANES)
                first = [fields_ref[2 * j + h, l, pl.ds(0, SUB), at] for h in range(2)]
                final = [fields_ref[2 * j + h, l, pl.ds(rows - SUB, SUB), at] for h in range(2)]
                ends[0, l, j, :, at] = jnp.where(sub < HALO, first[0], pltpu.roll(first[1], HALO, 0))
                ends[1, l, j, :, at] = jnp.where(sub < HALO, pltpu.roll(final[0], HALO, 0), final[1])
    pl.semaphore_wait(barrier, len(targets))

    copies = []

    def start_copy(source, dest, recv_sem, target):
        copy = pltpu.make_async_remote_copy(
            src_ref=source,
            dst_ref=dest,
            send_sem=send.at[len(copies)],
            recv_sem=recv_sem,
            device_id=target,
            device_id_type=pl.DeviceIdType.MESH,
        )
        copy.start()
        copies.append(copy)

    for k, (where, slot) in enumerate(((up, slot_up), (down, slot_down))):
        start_copy(ends.at[k], far.at[slot], recv.at[2 + slot], where)
    for k, step in enumerate((1, -1)):
        start_copy(edge.at[k], side.at[k], recv.at[k], ahead(here, step))
    for n, (where, slot) in enumerate(((up, slot_up), (down, slot_down))):
        span = pl.ds((rows - SUB) * n, SUB)
        for k, step in enumerate((1, -1)):
            start_copy(edge.at[k, span], near.at[k, slot], recv.at[4 + 2 * k + slot], ahead(where, step))
    for copy in copies:
        copy.wait_send()

    def arrived(dest, sem):
        pltpu.make_async_copy(dest, dest, recv.at[sem]).wait()

    for k in range(2):
        arrived(side.at[k], k)
        arrived(far.at[k], 2 + k)
        for n in range(2):
            arrived(near.at[k, n], 4 + 2 * k + n)
    gap = LANES - HALO - (cols - last)
    corner = []
    for k in range(2):
        north, south = near[k, 0], near[k, 1]
        north = jnp.where(top, pltpu.roll(north, HALO, 0), north)
        south = jnp.where(bottom, pltpu.roll(south, HALO, 0), south)
        corner.append(jnp.where(sub < HALO, south, north))
    for i in range(rows // SUB + 1):
        span = pl.ds(SUB * i, SUB)
        west, east = (side[k, span, :] if i < rows // SUB else corner[k] for k in range(2))
        for l in range(nlev):
            place = HALO * nfield * l
            moved = pltpu.roll(west, (gap - place) % LANES, 1)
            flank_ref[l, span, :] = jnp.where(lane < gap, pltpu.roll(east, LANES - place, 1) if l else east, moved)
    rows_ref[...] = far[...]


def halos(fields):
    nfield, nlev, rows, cols = fields.shape
    wide = pl.cdiv(cols, LANES) * LANES
    ends = (2, nlev, nfield // 2, SUB, wide)
    shapes = [(nlev, rows + SUB, LANES), ends]

    def whole(shape):
        return pl.BlockSpec(shape, lambda n: (0,) * len(shape))

    return pl.pallas_call(
        functools.partial(exchange, cols),
        grid=(1,),
        out_shape=[jax.ShapeDtypeStruct(s, jnp.float32) for s in shapes],
        in_specs=[whole((nfield, nlev, rows, wide))],
        out_specs=[whole(s) for s in shapes],
        scratch_shapes=[
            pltpu.VMEM((2, rows, LANES), jnp.float32),
            pltpu.VMEM(ends, jnp.float32),
            pltpu.VMEM((2, rows, LANES), jnp.float32),
            pltpu.VMEM(ends, jnp.float32),
            pltpu.VMEM((2, 2, SUB, LANES), jnp.float32),
            pltpu.SemaphoreType.DMA((8,)),
            pltpu.SemaphoreType.DMA((8,)),
        ],
        compiler_params=pltpu.CompilerParams(collective_id=0, has_side_effects=True),
    )(fields)


def body(fields, dep_row, dep_col, weights):
    nfield, nlev, rows, cols = fields.shape
    flank, ends = halos(fields)
    tiles = pl.cdiv(cols, LANES)
    wide = tiles * LANES
    assert nfield % 2 == 0 and HALO * nfield * nlev <= LANES - HALO
    assert rows % SUB == 0 and CHUNK * tiles >= cols and cols + 2 * HALO <= wide

    def block(lead, h, w):
        return pl.BlockSpec((lead, 1, h, w), lambda l: (0, l, 0, 0))

    point = pl.BlockSpec((1, rows, wide), lambda l: (l, 0, 0))
    return pl.pallas_call(
        functools.partial(stencil, cols, cols * lax.axis_size("lon")),
        grid=(nlev,),
        out_shape=jax.ShapeDtypeStruct(fields.shape, jnp.float32),
        in_specs=[
            block(nfield, rows, wide),
            point,
            point,
            block(8, rows, wide),
            pl.BlockSpec((1, rows + SUB, LANES), lambda l: (l, 0, 0)),
            pl.BlockSpec((2, 1, nfield // 2, SUB, wide), lambda l: (0, l, 0, 0, 0)),
        ],
        out_specs=block(nfield, rows, wide),
        scratch_shapes=[
            pltpu.VMEM((nfield, NSHIFT, tiles, rows + 2 * SUB, LANES), jnp.float32),
            pltpu.VMEM((2 * NSHIFT, tiles, rows, LANES), jnp.float32),
            pltpu.VMEM((nfield, tiles, rows, LANES), jnp.float32),
        ],
    )(fields, dep_row, dep_col, weights, flank, ends)


def solution(mesh):
    return jax.shard_map(
        body,
        mesh=mesh,
        in_specs=(
            P(None, None, "lat", "lon"),
            P(None, "lat", "lon"),
            P(None, "lat", "lon"),
            P(None, None, "lat", "lon"),
        ),
        out_specs=P(None, None, "lat", "lon"),
        check_vma=False,
    )
```

```python
import functools

import jax
import jax.numpy as jnp
from jax import lax
from jax.experimental import pallas as pl
from jax.experimental.pallas import tpu as pltpu
from jax.sharding import PartitionSpec as P

HALO = 4
LANES = 128
SUB = 8
CHUNK = LANES - 2 * HALO
NSHIFT = 2 * HALO


def lane_index():
    return lax.broadcasted_iota(jnp.int32, (SUB, LANES), 1)


def sublane_index():
    return lax.broadcasted_iota(jnp.int32, (SUB, LANES), 0)


def tile_of(view, t, cols):
    width = min(LANES, cols - LANES * t)
    value = view[:, pl.ds(LANES * t, width)]
    if width == LANES:
        return value
    return jnp.concatenate([value, jnp.zeros((SUB, LANES - width), value.dtype)], axis=1)


def chunked(tiles, side=None):
    lane = lane_index()
    out = [tiles[0] if side is None else jnp.where(lane < LANES - HALO, tiles[0], side)]
    for t in range(1, len(tiles)):
        back = (LANES - CHUNK) * t
        mixed = jnp.where(lane < LANES - HALO - back, tiles[t], tiles[t - 1])
        out.append(pltpu.roll(mixed, back, 1))
    return out


def unchunked(chunks):
    lane = lane_index()
    count = len(chunks)
    ahead = [c if t == 0 else pltpu.roll(c, LANES - (LANES - CHUNK) * t, 1) for t, c in enumerate(chunks)]
    return [
        ahead[t] if t == count - 1 else jnp.where(lane < CHUNK - (LANES - CHUNK) * t, ahead[t], ahead[t + 1])
        for t in range(count)
    ]


def spread(offset, w):
    one, two, four = (offset & 1) != 0, (offset & 2) != 0, offset == 4
    zero = jnp.zeros_like(w[0])
    u = [jnp.where(one, a, b) for a, b in zip([zero] + w, w + [zero])]
    v = [jnp.where(two, a, b) for a, b in zip([zero, zero] + u, u + [zero, zero])]
    return [jnp.where(four, a, b) for a, b in zip([zero] * 4 + w, v + [zero])]


def stencil(cols, total_cols, fields_ref, row_ref, col_ref, weight_ref, flank_ref, rows_ref, out_ref, xs, sel, res):
    nfield, rows = fields_ref.shape[0], fields_ref.shape[2]
    tiles = pl.cdiv(cols, LANES)
    groups = rows // SUB
    row0 = lax.axis_index("lat") * rows
    col0 = lax.axis_index("lon") * cols
    held = cols - LANES * (tiles - 1)
    lane, sub = lane_index(), sublane_index()
    top, bottom = lax.axis_index("lat") == 0, lax.axis_index("lat") == lax.axis_size("lat") - 1
    turned = ((sub < HALO) & bottom) | ((sub >= HALO) & top)
    lanes_of = [pl.ds(LANES * t, LANES) for t in range(tiles)]

    for i in range(groups):
        span = pl.ds(SUB * i, SUB)
        offsets = []
        for t in range(tiles):
            o_row = tile_of(row_ref.at[0, span], t, cols) - (row0 + SUB * i + sub) + HALO
            back = tile_of(col_ref.at[0, span], t, cols) - (col0 + LANES * t + lane)
            o_col = jnp.where(back > 0, back - total_cols, back) + HALO
            offsets.append(o_row * 16 + o_col)
        offsets = chunked(offsets)
        w = [chunked([tile_of(weight_ref.at[q, 0, span], t, cols) for t in range(tiles)]) for q in range(8)]
        for t in range(tiles):
            for base, offset in ((0, offsets[t] >> 4), (4, offsets[t] & 15)):
                slots = spread(offset, [w[base + a][t] for a in range(4)])
                for s in range(NSHIFT):
                    sel[2 * base + s, t, span, :] = slots[s]

    def shifted(f, t, chunk, places):
        for s in range(NSHIFT):
            value = chunk if s == HALO else pltpu.roll(chunk, (HALO - s) % LANES, 1)
            for i in places:
                xs[f, s, t, pl.ds(SUB * i, SUB), :] = value

    for f in range(nfield):
        def flanks(i):
            return pltpu.roll(flank_ref[0, pl.ds(SUB * i, SUB), :], held - HALO * f, 1)

        for i in range(groups):
            span = pl.ds(SUB * i, SUB)
            side = flanks(i)
            got = [tile_of(fields_ref.at[f, 0, span], t, cols) for t in range(tiles)]
            got[-1] = jnp.where(lane < held, got[-1], side)
            for t, chunk in enumerate(chunked(got, side)):
                shifted(f, t, chunk, (i + 1,))
        got = []
        for at in lanes_of:
            north, south = (rows_ref[n, 0, f // 2, :, at] for n in range(2))
            if f % 2 == 0:
                north = pltpu.roll(north, HALO, 0)
            else:
                south = pltpu.roll(south, HALO, 0)
            got.append(jnp.where(sub < HALO, south, north))
        got[-1] = jnp.where(lane < held, got[-1], flanks(groups))
        for t in range(tiles):
            back = got[t]
            for step in (1, 2):
                back = jnp.where((sub & step) != 0, pltpu.roll(back, step, 0), pltpu.roll(back, SUB - step, 0))
            got[t] = jnp.where(turned, back, got[t])
        for t, chunk in enumerate(chunked(got, got[-1])):
            shifted(f, t, chunk, (0, groups + 1))

    stride = rows // SUB
    many = 2 if stride % 2 == 0 else 1
    pair = 2 if nfield % 2 == 0 else 1
    def block(n, carry):
        f0, rest = pair * lax.rem(n, nfield // pair), n // (nfield // pair)
        m0, t = many * lax.rem(rest, stride // many), rest // (stride // many)
        rowsel = [[sel[r, t, pl.ds(m0 + m, SUB, stride=stride), :] for r in range(NSHIFT)] for m in range(many)]
        total = [[None] * pair for _ in range(many)]
        for s in range(NSHIFT):
            colsel = [sel[NSHIFT + s, t, pl.ds(m0 + m, SUB, stride=stride), :] for m in range(many)]
            for f in range(pair):
                x = [xs[f0 + f, s, t, pl.ds(HALO + m0 + r, SUB, stride=stride), :] for r in range(many + NSHIFT - 1)]
                for m in range(many):
                    line = rowsel[m][0] * x[m]
                    for r in range(1, NSHIFT):
                        line = line + rowsel[m][r] * x[m + r]
                    term = colsel[m] * line
                    total[m][f] = term if s == 0 else total[m][f] + term
        for m in range(many):
            for f in range(pair):
                res[f0 + f, t, pl.ds(m0 + m, SUB, stride=stride), :] = total[m][f]
        return carry

    lax.fori_loop(0, tiles * (stride // many) * (nfield // pair), block, 0)
    for f in range(nfield):
        for i in range(groups):
            span = pl.ds(SUB * i, SUB)
            for t, tile in enumerate(unchunked([res[f, t, span, :] for t in range(tiles)])):
                width = min(LANES, cols - LANES * t)
                out_ref[f, 0, span, pl.ds(LANES * t, width)] = tile[:, :width]


def exchange(cols, fields_ref, flank_ref, rows_ref, edge, ends, side, far, near, send, recv):
    nfield, nlev, rows = fields_ref.shape[:3]
    tiles = pl.cdiv(cols, LANES)
    last = LANES * (tiles - 1)
    lat_count, lon_count = lax.axis_size("lat"), lax.axis_size("lon")
    band, sector = lax.axis_index("lat"), lax.axis_index("lon")
    lane, sub = lane_index(), sublane_index()
    top, bottom = band == 0, band == lat_count - 1
    across = lax.rem(sector + lon_count // 2, lon_count)
    up = (jnp.maximum(band - 1, 0), jnp.where(top, across, sector))
    down = (jnp.minimum(band + 1, lat_count - 1), jnp.where(bottom, across, sector))
    slot_up, slot_down = jnp.where(top, 0, 1), jnp.where(bottom, 1, 0)

    def ahead(where, step):
        return (where[0], lax.rem(where[1] + step + lon_count, lon_count))

    here = (band, sector)
    targets = [ahead(here, 1), ahead(here, -1)]
    for where in (up, down):
        targets += [where, ahead(where, 1), ahead(where, -1)]
    barrier = pltpu.get_barrier_semaphore()
    for target in targets:
        pl.semaphore_signal(barrier, inc=1, device_id=target, device_id_type=pl.DeviceIdType.MESH)

    for i in range(rows // SUB):
        span = pl.ds(SUB * i, SUB)
        packed = [jnp.zeros((SUB, LANES), jnp.float32)] * 2
        for l in range(nlev):
            for f in range(nfield):
                g = HALO * (l * nfield + f)
                mine = (lane >= g) & (lane < g + HALO)
                ending = tile_of(fields_ref.at[f, l, span], tiles - 1, cols)
                start = fields_ref[f, l, span, pl.ds(0, LANES)]
                shift = (g - (cols - last - HALO)) % LANES
                packed[0] = jnp.where(mine, pltpu.roll(ending, shift, 1) if shift else ending, packed[0])
                packed[1] = jnp.where(mine, pltpu.roll(start, g, 1) if g else start, packed[1])
        for k in range(2):
            edge[k, span, :] = packed[k]
    for l in range(nlev):
        for j in range(nfield // 2):
            for t in range(tiles):
                at = pl.ds(LANES * t, LANES)
                first = [tile_of(fields_ref.at[2 * j + h, l, pl.ds(0, SUB)], t, cols) for h in range(2)]
                final = [tile_of(fields_ref.at[2 * j + h, l, pl.ds(rows - SUB, SUB)], t, cols) for h in range(2)]
                ends[0, l, j, :, at] = jnp.where(sub < HALO, first[0], pltpu.roll(first[1], HALO, 0))
                ends[1, l, j, :, at] = jnp.where(sub < HALO, pltpu.roll(final[0], HALO, 0), final[1])
    pl.semaphore_wait(barrier, len(targets))

    copies = []

    def start_copy(source, dest, recv_sem, target):
        copy = pltpu.make_async_remote_copy(
            src_ref=source,
            dst_ref=dest,
            send_sem=send.at[len(copies)],
            recv_sem=recv_sem,
            device_id=target,
            device_id_type=pl.DeviceIdType.MESH,
        )
        copy.start()
        copies.append(copy)

    for k, (where, slot) in enumerate(((up, slot_up), (down, slot_down))):
        start_copy(ends.at[k], far.at[slot], recv.at[2 + slot], where)
    for k, step in enumerate((1, -1)):
        start_copy(edge.at[k], side.at[k], recv.at[k], ahead(here, step))
    for n, (where, slot) in enumerate(((up, slot_up), (down, slot_down))):
        span = pl.ds((rows - SUB) * n, SUB)
        for k, step in enumerate((1, -1)):
            start_copy(edge.at[k, span], near.at[k, slot], recv.at[4 + 2 * k + slot], ahead(where, step))
    for copy in copies:
        copy.wait_send()

    def arrived(dest, sem):
        pltpu.make_async_copy(dest, dest, recv.at[sem]).wait()

    for k in range(2):
        arrived(side.at[k], k)
        arrived(far.at[k], 2 + k)
        for n in range(2):
            arrived(near.at[k, n], 4 + 2 * k + n)
    gap = LANES - HALO - (cols - last)
    corner = []
    for k in range(2):
        north, south = near[k, 0], near[k, 1]
        north = jnp.where(top, pltpu.roll(north, HALO, 0), north)
        south = jnp.where(bottom, pltpu.roll(south, HALO, 0), south)
        corner.append(jnp.where(sub < HALO, south, north))
    for i in range(rows // SUB + 1):
        span = pl.ds(SUB * i, SUB)
        west, east = (side[k, span, :] if i < rows // SUB else corner[k] for k in range(2))
        for l in range(nlev):
            place = HALO * nfield * l
            moved = pltpu.roll(west, (gap - place) % LANES, 1)
            flank_ref[l, span, :] = jnp.where(lane < gap, pltpu.roll(east, LANES - place, 1) if l else east, moved)
    rows_ref[...] = far[...]


def halos(fields):
    nfield, nlev, rows, cols = fields.shape
    wide = pl.cdiv(cols, LANES) * LANES
    ends = (2, nlev, nfield // 2, SUB, wide)
    shapes = [(nlev, rows + SUB, LANES), ends]

    def whole(shape):
        return pl.BlockSpec(shape, lambda n: (0,) * len(shape))

    return pl.pallas_call(
        functools.partial(exchange, cols),
        grid=(1,),
        out_shape=[jax.ShapeDtypeStruct(s, jnp.float32) for s in shapes],
        in_specs=[whole(fields.shape)],
        out_specs=[whole(s) for s in shapes],
        scratch_shapes=[
            pltpu.VMEM((2, rows, LANES), jnp.float32),
            pltpu.VMEM(ends, jnp.float32),
            pltpu.VMEM((2, rows, LANES), jnp.float32),
            pltpu.VMEM(ends, jnp.float32),
            pltpu.VMEM((2, 2, SUB, LANES), jnp.float32),
            pltpu.SemaphoreType.DMA((8,)),
            pltpu.SemaphoreType.DMA((8,)),
        ],
        compiler_params=pltpu.CompilerParams(collective_id=0, has_side_effects=True),
    )(fields)


def body(fields, dep_row, dep_col, weights):
    nfield, nlev, rows, cols = fields.shape
    flank, ends = halos(fields)
    tiles = pl.cdiv(cols, LANES)
    wide = tiles * LANES
    assert nfield % 2 == 0 and HALO * nfield * nlev <= LANES - HALO
    assert rows % SUB == 0 and CHUNK * tiles >= cols and cols + 2 * HALO <= wide

    def block(lead, h, w):
        return pl.BlockSpec((lead, 1, h, w), lambda l: (0, l, 0, 0))

    point = pl.BlockSpec((1, rows, cols), lambda l: (l, 0, 0))
    return pl.pallas_call(
        functools.partial(stencil, cols, cols * lax.axis_size("lon")),
        grid=(nlev,),
        out_shape=jax.ShapeDtypeStruct(fields.shape, jnp.float32),
        in_specs=[
            block(nfield, rows, cols),
            point,
            point,
            block(8, rows, cols),
            pl.BlockSpec((1, rows + SUB, LANES), lambda l: (l, 0, 0)),
            pl.BlockSpec((2, 1, nfield // 2, SUB, wide), lambda l: (0, l, 0, 0, 0)),
        ],
        out_specs=block(nfield, rows, cols),
        scratch_shapes=[
            pltpu.VMEM((nfield, NSHIFT, tiles, rows + 2 * SUB, LANES), jnp.float32),
            pltpu.VMEM((2 * NSHIFT, tiles, rows, LANES), jnp.float32),
            pltpu.VMEM((nfield, tiles, rows, LANES), jnp.float32),
        ],
    )(fields, dep_row, dep_col, weights, flank, ends)


def solution(mesh):
    return jax.shard_map(
        body,
        mesh=mesh,
        in_specs=(
            P(None, None, "lat", "lon"),
            P(None, "lat", "lon"),
            P(None, "lat", "lon"),
            P(None, None, "lat", "lon"),
        ),
        out_specs=P(None, None, "lat", "lon"),
        check_vma=False,
    )
```

```python
import functools

import jax
import jax.numpy as jnp
from jax import lax
from jax.experimental import pallas as pl
from jax.experimental.pallas import tpu as pltpu
from jax.sharding import PartitionSpec as P

HALO = 4
LANES = 128
SUB = 8
CHUNK = LANES - 2 * HALO
NSHIFT = 2 * HALO


def lane_index():
    return lax.broadcasted_iota(jnp.int32, (SUB, LANES), 1)


def sublane_index():
    return lax.broadcasted_iota(jnp.int32, (SUB, LANES), 0)


def tile_of(view, t, cols):
    width = min(LANES, cols - LANES * t)
    value = view[:, pl.ds(LANES * t, width)]
    if width == LANES:
        return value
    return jnp.concatenate([value, jnp.zeros((SUB, LANES - width), value.dtype)], axis=1)


def chunked(tiles, side=None):
    lane = lane_index()
    out = [tiles[0] if side is None else jnp.where(lane < LANES - HALO, tiles[0], side)]
    for t in range(1, len(tiles)):
        back = (LANES - CHUNK) * t
        mixed = jnp.where(lane < LANES - HALO - back, tiles[t], tiles[t - 1])
        out.append(pltpu.roll(mixed, back, 1))
    return out


def unchunked(chunks):
    lane = lane_index()
    count = len(chunks)
    ahead = [c if t == 0 else pltpu.roll(c, LANES - (LANES - CHUNK) * t, 1) for t, c in enumerate(chunks)]
    return [
        ahead[t] if t == count - 1 else jnp.where(lane < CHUNK - (LANES - CHUNK) * t, ahead[t], ahead[t + 1])
        for t in range(count)
    ]


def spread(offset, w):
    one, two, four = (offset & 1) != 0, (offset & 2) != 0, offset == 4
    zero = jnp.zeros_like(w[0])
    u = [jnp.where(one, a, b) for a, b in zip([zero] + w, w + [zero])]
    v = [jnp.where(two, a, b) for a, b in zip([zero, zero] + u, u + [zero, zero])]
    return [jnp.where(four, a, b) for a, b in zip([zero] * 4 + w, v + [zero])]


def stencil(cols, total_cols, fields_ref, row_ref, col_ref, weight_ref, flank_ref, rows_ref, out_ref, xs, sel, res):
    nfield, rows = fields_ref.shape[0], fields_ref.shape[2]
    tiles = pl.cdiv(cols, LANES)
    groups = rows // SUB
    row0 = lax.axis_index("lat") * rows
    col0 = lax.axis_index("lon") * cols
    held = cols - LANES * (tiles - 1)
    lane, sub = lane_index(), sublane_index()
    top, bottom = lax.axis_index("lat") == 0, lax.axis_index("lat") == lax.axis_size("lat") - 1
    turned = ((sub < HALO) & bottom) | ((sub >= HALO) & top)
    lanes_of = [pl.ds(LANES * t, LANES) for t in range(tiles)]

    for i in range(groups):
        span = pl.ds(SUB * i, SUB)
        offsets = []
        for t in range(tiles):
            o_row = tile_of(row_ref.at[0, span], t, cols) - (row0 + SUB * i + sub) + HALO
            back = tile_of(col_ref.at[0, span], t, cols) - (col0 + LANES * t + lane)
            o_col = jnp.where(back > 0, back - total_cols, back) + HALO
            offsets.append(o_row * 16 + o_col)
        offsets = chunked(offsets)
        w = [chunked([tile_of(weight_ref.at[q, 0, span], t, cols) for t in range(tiles)]) for q in range(8)]
        for t in range(tiles):
            for base, offset in ((0, offsets[t] >> 4), (4, offsets[t] & 15)):
                slots = spread(offset, [w[base + a][t] for a in range(4)])
                for s in range(NSHIFT):
                    sel[2 * base + s, t, span, :] = slots[s]

    def shifted(f, t, chunk, places):
        for s in range(NSHIFT):
            value = chunk if s == HALO else pltpu.roll(chunk, (HALO - s) % LANES, 1)
            for i in places:
                xs[f, s, t, pl.ds(SUB * i, SUB), :] = value

    for f in range(nfield):
        def flanks(i):
            return pltpu.roll(flank_ref[0, pl.ds(SUB * i, SUB), :], held - HALO * f, 1)

        for i in range(groups):
            span = pl.ds(SUB * i, SUB)
            side = flanks(i)
            got = [tile_of(fields_ref.at[f, 0, span], t, cols) for t in range(tiles)]
            got[-1] = jnp.where(lane < held, got[-1], side)
            for t, chunk in enumerate(chunked(got, side)):
                shifted(f, t, chunk, (i + 1,))
        got = []
        for at in lanes_of:
            north, south = (rows_ref[n, 0, f // 2, :, at] for n in range(2))
            if f % 2 == 0:
                north = pltpu.roll(north, HALO, 0)
            else:
                south = pltpu.roll(south, HALO, 0)
            got.append(jnp.where(sub < HALO, south, north))
        got[-1] = jnp.where(lane < held, got[-1], flanks(groups))
        for t in range(tiles):
            back = got[t]
            for step in (1, 2):
                back = jnp.where((sub & step) != 0, pltpu.roll(back, step, 0), pltpu.roll(back, SUB - step, 0))
            got[t] = jnp.where(turned, back, got[t])
        for t, chunk in enumerate(chunked(got, got[-1])):
            shifted(f, t, chunk, (0, groups + 1))

    stride = rows // SUB
    many = 2 if stride % 2 == 0 else 1
    pair = 2 if nfield % 2 == 0 else 1
    def block(n, carry):
        f0, rest = pair * lax.rem(n, nfield // pair), n // (nfield // pair)
        m0, t = many * lax.rem(rest, stride // many), rest // (stride // many)
        rowsel = [[sel[r, t, pl.ds(m0 + m, SUB, stride=stride), :] for r in range(NSHIFT)] for m in range(many)]
        total = [[None] * pair for _ in range(many)]
        for s in range(NSHIFT):
            colsel = [sel[NSHIFT + s, t, pl.ds(m0 + m, SUB, stride=stride), :] for m in range(many)]
            for f in range(pair):
                x = [xs[f0 + f, s, t, pl.ds(HALO + m0 + r, SUB, stride=stride), :] for r in range(many + NSHIFT - 1)]
                for m in range(many):
                    line = rowsel[m][0] * x[m]
                    for r in range(1, NSHIFT):
                        line = line + rowsel[m][r] * x[m + r]
                    term = colsel[m] * line
                    total[m][f] = term if s == 0 else total[m][f] + term
        for m in range(many):
            for f in range(pair):
                res[f0 + f, t, pl.ds(m0 + m, SUB, stride=stride), :] = total[m][f]
        return carry

    lax.fori_loop(0, tiles * (stride // many) * (nfield // pair), block, 0)
    for f in range(nfield):
        for i in range(groups):
            span = pl.ds(SUB * i, SUB)
            for t, tile in enumerate(unchunked([res[f, t, span, :] for t in range(tiles)])):
                width = min(LANES, cols - LANES * t)
                out_ref[f, 0, span, pl.ds(LANES * t, width)] = tile[:, :width]


def exchange(cols, fields_ref, flank_ref, rows_ref, edge, ends, side, far, near, send, recv):
    nfield, nlev, rows = fields_ref.shape[:3]
    tiles = pl.cdiv(cols, LANES)
    last = LANES * (tiles - 1)
    lat_count, lon_count = lax.axis_size("lat"), lax.axis_size("lon")
    band, sector = lax.axis_index("lat"), lax.axis_index("lon")
    lane, sub = lane_index(), sublane_index()
    top, bottom = band == 0, band == lat_count - 1
    across = lax.rem(sector + lon_count // 2, lon_count)
    up = (jnp.maximum(band - 1, 0), jnp.where(top, across, sector))
    down = (jnp.minimum(band + 1, lat_count - 1), jnp.where(bottom, across, sector))
    slot_up, slot_down = jnp.where(top, 0, 1), jnp.where(bottom, 1, 0)

    def ahead(where, step):
        return (where[0], lax.rem(where[1] + step + lon_count, lon_count))

    here = (band, sector)
    targets = [ahead(here, 1), ahead(here, -1)]
    for where in (up, down):
        targets += [where, ahead(where, 1), ahead(where, -1)]
    barrier = pltpu.get_barrier_semaphore()
    for target in targets:
        pl.semaphore_signal(barrier, inc=1, device_id=target, device_id_type=pl.DeviceIdType.MESH)

    for i in range(rows // SUB):
        span = pl.ds(SUB * i, SUB)
        packed = [jnp.zeros((SUB, LANES), jnp.float32)] * 2
        for l in range(nlev):
            for f in range(nfield):
                g = HALO * (l * nfield + f)
                mine = (lane >= g) & (lane < g + HALO)
                ending = tile_of(fields_ref.at[f, l, span], tiles - 1, cols)
                start = fields_ref[f, l, span, pl.ds(0, LANES)]
                shift = (g - (cols - last - HALO)) % LANES
                packed[0] = jnp.where(mine, pltpu.roll(ending, shift, 1) if shift else ending, packed[0])
                packed[1] = jnp.where(mine, pltpu.roll(start, g, 1) if g else start, packed[1])
        for k in range(2):
            edge[k, span, :] = packed[k]
    for l in range(nlev):
        for j in range(nfield // 2):
            for t in range(tiles):
                at = pl.ds(LANES * t, LANES)
                first = [tile_of(fields_ref.at[2 * j + h, l, pl.ds(0, SUB)], t, cols) for h in range(2)]
                final = [tile_of(fields_ref.at[2 * j + h, l, pl.ds(rows - SUB, SUB)], t, cols) for h in range(2)]
                ends[0, l, j, :, at] = jnp.where(sub < HALO, first[0], pltpu.roll(first[1], HALO, 0))
                ends[1, l, j, :, at] = jnp.where(sub < HALO, pltpu.roll(final[0], HALO, 0), final[1])
    pl.semaphore_wait(barrier, len(targets))

    copies = []

    def start_copy(source, dest, recv_sem, target):
        copy = pltpu.make_async_remote_copy(
            src_ref=source,
            dst_ref=dest,
            send_sem=send.at[len(copies)],
            recv_sem=recv_sem,
            device_id=target,
            device_id_type=pl.DeviceIdType.MESH,
        )
        copy.start()
        copies.append(copy)

    for k, (where, slot) in enumerate(((up, slot_up), (down, slot_down))):
        start_copy(ends.at[k], far.at[slot], recv.at[2 + slot], where)
    for k, step in enumerate((1, -1)):
        start_copy(edge.at[k], side.at[k], recv.at[k], ahead(here, step))
    for n, (where, slot) in enumerate(((up, slot_up), (down, slot_down))):
        span = pl.ds((rows - SUB) * n, SUB)
        for k, step in enumerate((1, -1)):
            start_copy(edge.at[k, span], near.at[k, slot], recv.at[4 + 2 * k + slot], ahead(where, step))
    for copy in copies:
        copy.wait_send()

    def arrived(dest, sem):
        pltpu.make_async_copy(dest, dest, recv.at[sem]).wait()

    for k in range(2):
        arrived(side.at[k], k)
        arrived(far.at[k], 2 + k)
        for n in range(2):
            arrived(near.at[k, n], 4 + 2 * k + n)
    gap = LANES - HALO - (cols - last)
    corner = []
    for k in range(2):
        north, south = near[k, 0], near[k, 1]
        north = jnp.where(top, pltpu.roll(north, HALO, 0), north)
        south = jnp.where(bottom, pltpu.roll(south, HALO, 0), south)
        corner.append(jnp.where(sub < HALO, south, north))
    for i in range(rows // SUB + 1):
        span = pl.ds(SUB * i, SUB)
        west, east = (side[k, span, :] if i < rows // SUB else corner[k] for k in range(2))
        for l in range(nlev):
            place = HALO * nfield * l
            moved = pltpu.roll(west, (gap - place) % LANES, 1)
            flank_ref[l, span, :] = jnp.where(lane < gap, pltpu.roll(east, LANES - place, 1) if l else east, moved)
    rows_ref[...] = far[...]


def halos(fields):
    nfield, nlev, rows, cols = fields.shape
    wide = pl.cdiv(cols, LANES) * LANES
    ends = (2, nlev, nfield // 2, SUB, wide)
    shapes = [(nlev, rows + SUB, LANES), ends]

    def whole(shape):
        return pl.BlockSpec(shape, lambda n: (0,) * len(shape))

    return pl.pallas_call(
        functools.partial(exchange, cols),
        grid=(1,),
        out_shape=[jax.ShapeDtypeStruct(s, jnp.float32) for s in shapes],
        in_specs=[whole(fields.shape)],
        out_specs=[whole(s) for s in shapes],
        scratch_shapes=[
            pltpu.VMEM((2, rows, LANES), jnp.float32),
            pltpu.VMEM(ends, jnp.float32),
            pltpu.VMEM((2, rows, LANES), jnp.float32),
            pltpu.VMEM(ends, jnp.float32),
            pltpu.VMEM((2, 2, SUB, LANES), jnp.float32),
            pltpu.SemaphoreType.DMA((8,)),
            pltpu.SemaphoreType.DMA((8,)),
        ],
        cost_estimate=pl.CostEstimate(flops=0, bytes_accessed=40_000_000, transcendentals=0),
        compiler_params=pltpu.CompilerParams(collective_id=0, has_side_effects=True, vmem_limit_bytes=16 << 20),
    )(fields)


def body(fields, dep_row, dep_col, weights):
    nfield, nlev, rows, cols = fields.shape
    flank, ends = halos(fields)
    tiles = pl.cdiv(cols, LANES)
    wide = tiles * LANES
    assert nfield % 2 == 0 and HALO * nfield * nlev <= LANES - HALO
    assert rows % SUB == 0 and CHUNK * tiles >= cols and cols + 2 * HALO <= wide

    def block(lead, h, w):
        return pl.BlockSpec((lead, 1, h, w), lambda l: (0, l, 0, 0))

    point = pl.BlockSpec((1, rows, cols), lambda l: (l, 0, 0))
    return pl.pallas_call(
        functools.partial(stencil, cols, cols * lax.axis_size("lon")),
        grid=(nlev,),
        out_shape=jax.ShapeDtypeStruct(fields.shape, jnp.float32),
        in_specs=[
            block(nfield, rows, cols),
            point,
            point,
            block(8, rows, cols),
            pl.BlockSpec((1, rows + SUB, LANES), lambda l: (l, 0, 0)),
            pl.BlockSpec((2, 1, nfield // 2, SUB, wide), lambda l: (0, l, 0, 0, 0)),
        ],
        out_specs=block(nfield, rows, cols),
        scratch_shapes=[
            pltpu.VMEM((nfield, NSHIFT, tiles, rows + 2 * SUB, LANES), jnp.float32),
            pltpu.VMEM((2 * NSHIFT, tiles, rows, LANES), jnp.float32),
            pltpu.VMEM((nfield, tiles, rows, LANES), jnp.float32),
        ],
    )(fields, dep_row, dep_col, weights, flank, ends)


def solution(mesh):
    return jax.shard_map(
        body,
        mesh=mesh,
        in_specs=(
            P(None, None, "lat", "lon"),
            P(None, "lat", "lon"),
            P(None, "lat", "lon"),
            P(None, None, "lat", "lon"),
        ),
        out_specs=P(None, None, "lat", "lon"),
        check_vma=False,
    )
```
